32 devices in a mesh: gz: 2 (over core), row: 4 (over y, x), col: 4 (over z).
Axes of the slice: x: 2, y: 2, z: 4, core: 2. Of those that a mesh axis runs over, the one named last changes fastest.
Arguments:
- rhs_sub: float32 [2, 3, 4, 96, 256], P('gz', None, 'row', 'col'), may hold values from -6 to 6
- rhs_top: float32 [2, 4, 96, 256], P(None, 'row', 'col'), may hold values from -6 to 6
- lower_sub: bfloat16 [2, 3, 4, 4, 256, 256], P('gz', None, 'row', 'col'), may hold values from -0.078125 to 0.078125
- lower_link: bfloat16 [2, 2, 4, 4, 256, 256], P('gz', None, 'row', 'col'), may hold values from -0.078125 to 0.078125
- lower_top: bfloat16 [1, 4, 4, 256, 256], P(None, 'row', 'col'), may hold values from -0.078125 to 0.078125
- inv_sub: bfloat16 [2, 3, 4, 256, 256], P('gz', None, 'row'), may hold values from -0.3 to 1.3
- inv_top: bfloat16 [2, 4, 256, 256], P(None, 'row'), may hold values from -0.3 to 1.3
- mask_sub: int32 [2, 3, 4, 4], P('gz', None, 'row', 'col'), may hold values 0 or 1
- mask_link: int32 [2, 2, 4, 4], P('gz', None, 'row', 'col'), may hold values 0 or 1
- mask_top: int32 [1, 4, 4], P(None, 'row', 'col'), may hold values 0 or 1
Outputs:
- sol_sub: float32 [2, 3, 4, 96, 256], P('gz', None, 'row', 'col')
- sol_top: float32 [2, 4, 96, 256], P(None, 'row', 'col')
The draws below stay inside these ranges and needn't reach their ends.
All inputs are finite; a program needn't handle non-finite values. No bound on the sum of `mask_sub` or of `mask_link` or of `mask_top` on one device may be relied on, other than what follows from the above.
Results may differ from the reference program's by a relative error of at most 0.02.
Values may be sent and summed in bfloat16 or wider, within the bound.
No kernel may reach another device: no remote copies, remote signals or barrier semaphores. Data moves between devices by JAX's collectives and lax.ppermute only.
A program may use at most 64 MiB of HBM per device.

```python
import math
import jax
import jax.numpy as jnp
from jax import lax

B = 256
NRHS = 96
SUBL = 3
TOPL = 2
GROUPS = 2
NBL = 4
PAIRS = 3
TPAIRS = 1


def draw_inv_sub(key, part):
    block_shape = (GROUPS, SUBL, NBL, B, B)
    noise_draw = jax.random.truncated_normal(key, -4.0, 4.0, block_shape, jnp.float32)
    return (jnp.eye(B, dtype=jnp.float32) + 0.4 * noise_draw / math.sqrt(B)).astype(jnp.bfloat16)


def draw_inv_top(key, part):
    block_shape = (TOPL, NBL, B, B)
    noise_draw = jax.random.truncated_normal(key, -4.0, 4.0, block_shape, jnp.float32)
    return (jnp.eye(B, dtype=jnp.float32) + 0.4 * noise_draw / math.sqrt(B)).astype(jnp.bfloat16)


def touch_ends(values, rng, smallest, top_value):
    longest = values.shape.index(max(values.shape))
    spots = []
    for shift in (0, 1):
        where = [jax.random.randint(jax.random.fold_in(rng, axis), (), 0, length) for axis, length in enumerate(values.shape)]
        where[longest] = (where[longest] + shift) % values.shape[longest]
        spots.append(tuple(where))
    return values.at[spots[0]].set(smallest).at[spots[1]].set(top_value)


def shard_levels(key, extent, pieces, least, high):
    loudness, own = 1.0, jax.random.fold_in(key, 6)
    for axis_at, blocks in pieces:
        steps = jnp.exp(jax.random.uniform(jax.random.fold_in(own, axis_at), (blocks,), jnp.float32, least / len(pieces), high / len(pieces)))
        loudness = loudness * jnp.repeat(steps, extent[axis_at] // blocks).reshape([-1 if axis == axis_at else 1 for axis in range(len(extent))])
    return loudness


def scatter_about(rng, dims, width, reach, pieces=(), held_as=jnp.bfloat16):
    values = width * jax.random.normal(rng, dims, jnp.float32)
    if pieces:
        values = values * shard_levels(rng, dims, pieces, -0.22, 0.18)
    return jnp.clip(values, -reach, reach).astype(held_as)


def setup_inputs(seed: int = 0) -> dict:
    seeds = jax.random.split(jax.random.key(seed), 11)
    return {
        "rhs_sub": scatter_about(seeds[0], (GROUPS, SUBL, NBL, NRHS, B), 1.0, 6.0, ((0, 2), (2, 4), (3, 4)), jnp.float32),
        "rhs_top": scatter_about(seeds[1], (TOPL, NBL, NRHS, B), 1.0, 6.0, ((1, 4), (2, 4)), jnp.float32),
        "lower_sub": scatter_about(seeds[2], (GROUPS, PAIRS, NBL, NBL, B, B), (2 * B * NBL * SUBL) ** -0.5, 0.078125, ((0, 2), (2, 4), (3, 4))),
        "lower_link": scatter_about(seeds[3], (GROUPS, TOPL, NBL, NBL, B, B), (2 * B * NBL * SUBL) ** -0.5, 0.078125, ((0, 2), (2, 4), (3, 4))),
        "lower_top": scatter_about(seeds[4], (TPAIRS, NBL, NBL, B, B), (2 * B * NBL * SUBL) ** -0.5, 0.078125, ((1, 4), (2, 4))),
        "inv_sub": draw_inv_sub(jax.random.fold_in(seeds[10], 71), 0),
        "inv_top": draw_inv_top(jax.random.fold_in(seeds[10], 71), 0),
        "mask_sub": touch_ends((jax.random.randint(seeds[7], (GROUPS, PAIRS, NBL, NBL), 0, 4) < 3).astype(jnp.int32), jax.random.fold_in(seeds[7], 1), 0, 1),
        "mask_link": touch_ends((jax.random.randint(seeds[8], (GROUPS, TOPL, NBL, NBL), 0, 4) < 3).astype(jnp.int32), jax.random.fold_in(seeds[8], 1), 0, 1),
        "mask_top": touch_ends((jax.random.randint(seeds[9], (TPAIRS, NBL, NBL), 0, 4) < 3).astype(jnp.int32), jax.random.fold_in(seeds[9], 1), 0, 1),
    }


def pair_of(later_level, earlier):
    return later_level * (later_level - 1) // 2 + earlier


def to_half(values):
    return lax.optimization_barrier(values.astype(jnp.bfloat16))


def masked(blocks, pattern):
    return blocks.astype(jnp.float32) * pattern.astype(jnp.float32)[:, :, None, None]


def forward_apply(vectors, blocks, pattern):
    return jnp.einsum("jnb,ijbd->ind", vectors.astype(jnp.float32), masked(blocks, pattern))


def backward_apply(vectors, blocks, pattern):
    return jnp.einsum("knd,kjbd->jnb", vectors.astype(jnp.float32), masked(blocks, pattern))


def solve_rows(residual, inverse):
    rounded = to_half(residual).astype(jnp.float32)
    return jnp.einsum("inb,ibd->ind", rounded, inverse.astype(jnp.float32))


def solve_cols(residual, inverse):
    rounded = to_half(residual).astype(jnp.float32)
    return jnp.einsum("ind,ibd->inb", rounded, inverse.astype(jnp.float32))


def reference(rhs_sub, rhs_top, lower_sub, lower_link, lower_top, inv_sub, inv_top, mask_sub, mask_link, mask_top):
    sub_solved = []
    sub_half = []
    for group_index in range(GROUPS):
        solved_list = []
        half_list = []
        for tier_index in range(SUBL):
            partial_sum = jnp.zeros((NBL, NRHS, B), jnp.float32)
            for earlier in range(tier_index):
                pair_index = pair_of(tier_index, earlier)
                partial_sum = partial_sum + forward_apply(half_list[earlier], lower_sub[group_index, pair_index], mask_sub[group_index, pair_index])
            solved = solve_rows(rhs_sub[group_index, tier_index] - partial_sum, inv_sub[group_index, tier_index])
            solved_list.append(solved)
            half_list.append(to_half(solved))
        sub_solved.append(solved_list)
        sub_half.append(half_list)
    top_solved = []
    top_half = []
    for top_level in range(TOPL):
        partial_sum = jnp.zeros((NBL, NRHS, B), jnp.float32)
        for group_index in range(GROUPS):
            partial_sum = partial_sum + forward_apply(sub_half[group_index][SUBL - 1], lower_link[group_index, top_level], mask_link[group_index, top_level])
        for earlier in range(top_level):
            pair_index = pair_of(top_level, earlier)
            partial_sum = partial_sum + forward_apply(top_half[earlier], lower_top[pair_index], mask_top[pair_index])
        solved = solve_rows(rhs_top[top_level] - partial_sum, inv_top[top_level])
        top_solved.append(solved)
        top_half.append(to_half(solved))
    top_answer = [None] * TOPL
    top_answer_half = [None] * TOPL
    for top_level in reversed(range(TOPL)):
        partial_sum = jnp.zeros((NBL, NRHS, B), jnp.float32)
        for later_level in range(top_level + 1, TOPL):
            pair_index = pair_of(later_level, top_level)
            partial_sum = partial_sum + backward_apply(top_answer_half[later_level], lower_top[pair_index], mask_top[pair_index])
        answer = solve_cols(top_solved[top_level] - partial_sum, inv_top[top_level])
        top_answer[top_level] = answer
        top_answer_half[top_level] = to_half(answer)
    sub_answer = []
    for group_index in range(GROUPS):
        answers = [None] * SUBL
        answers_half = [None] * SUBL
        for tier_index in reversed(range(SUBL)):
            partial_sum = jnp.zeros((NBL, NRHS, B), jnp.float32)
            for later_level in range(tier_index + 1, SUBL):
                pair_index = pair_of(later_level, tier_index)
                partial_sum = partial_sum + backward_apply(answers_half[later_level], lower_sub[group_index, pair_index], mask_sub[group_index, pair_index])
            if tier_index == SUBL - 1:
                for top_level in range(TOPL):
                    partial_sum = partial_sum + backward_apply(top_answer_half[top_level], lower_link[group_index, top_level], mask_link[group_index, top_level])
            answer = solve_cols(sub_solved[group_index][tier_index] - partial_sum, inv_sub[group_index, tier_index])
            answers[tier_index] = answer
            answers_half[tier_index] = to_half(answer)
        sub_answer.append(jnp.stack(answers))
    return jnp.stack(sub_answer), jnp.stack(top_answer)
```

```python
import jax
import jax.numpy as jnp
from jax import lax
from jax.sharding import PartitionSpec as P

BF = jnp.bfloat16
F32 = jnp.float32


def ring_from(values, axis, step):
    size = lax.axis_size(axis)
    if step == 0:
        return values
    return lax.ppermute(values, axis, [((d + step) % size, d) for d in range(size)])


def rolled(stack, start):
    size = stack.shape[0]
    return lax.dynamic_slice_in_dim(jnp.concatenate([stack, stack]), start % size, size, 0)


def row_gather(block):
    return [ring_from(block, "row", p) for p in range(lax.axis_size("row"))]


def scaled(lower, pattern, inverse):
    kept = lower * pattern.astype(BF)[:, :, None, None]
    return jnp.einsum("ijbd,ide->ijbe", kept, inverse, preferred_element_type=F32).astype(BF)


def spread(vectors, gathered):
    return jnp.stack(
        [jnp.einsum("jnb,ijbd->ind", vectors, g, preferred_element_type=F32) for g in gathered]
    )


def to_owners(parts, levels):
    rows, cols = lax.axis_size("row"), lax.axis_size("col")
    r, j = lax.axis_index("row"), lax.axis_index("col")
    parts = parts.astype(BF)
    if rows == cols:
        total = lax.dynamic_index_in_dim(parts, (j - r) % rows, 0, False).astype(F32)
        for s in range(1, cols):
            send = lax.dynamic_index_in_dim(parts, (j + s - r) % rows, 0, False)
            got = lax.ppermute(send, "col", [(d, (d + s) % cols) for d in range(cols)])
            total = total + got.astype(F32)
        return total
    natural = rolled(parts, rows - r)
    natural = jnp.moveaxis(natural, 1, 2)
    natural = natural.reshape((cols, -1) + natural.shape[2:])
    got = lax.all_to_all(natural, "col", 0, 0, tiled=True)
    return jnp.moveaxis(jnp.sum(got.astype(F32), axis=0), 1, 0)


def from_owners(vectors):
    rows, cols = lax.axis_size("row"), lax.axis_size("col")
    r, j = lax.axis_index("row"), lax.axis_index("col")
    if rows == cols:
        stack = jnp.stack([ring_from(vectors, "col", s) for s in range(cols)])
        return rolled(stack, r - j)
    stack = lax.all_gather(vectors, "col", axis=1, tiled=True)
    stack = stack.reshape((stack.shape[0], rows, -1) + stack.shape[2:])
    return rolled(jnp.moveaxis(stack, 1, 0), r)


def collect(rel, index, gathered):
    total = 0.0
    for p, g in enumerate(gathered):
        total = total + jnp.einsum("knd,kjbd->jnb", rel[p, index], g, preferred_element_type=F32)
    return total


def owner_pairs(rows, cols):
    wide = cols // rows
    return [
        (a * cols + c, (c % rows) * cols + a * wide + c // rows)
        for a in range(rows)
        for c in range(cols)
    ]


def into_owner_layout(values, col_blocks):
    rows, cols = lax.axis_size("row"), lax.axis_size("col")
    if rows != cols:
        c = lax.axis_index("col")
        values = lax.all_gather(values, "col", axis=2, tiled=True)
        n = values.shape[2] // rows
        values = lax.dynamic_slice_in_dim(values, (c // rows) * col_blocks, col_blocks, 1)
        values = lax.dynamic_slice_in_dim(values, (c % rows) * n, n, 2)
    return lax.ppermute(values, ("row", "col"), owner_pairs(rows, cols))


def from_owner_layout(values, share):
    rows, cols = lax.axis_size("row"), lax.axis_size("col")
    values = lax.ppermute(values, ("row", "col"), [(b, a) for a, b in owner_pairs(rows, cols)])
    if rows != cols:
        every = lax.all_gather(values, "col", axis=0)
        every = every.reshape((cols // rows, rows) + every.shape[1:])
        every = every.transpose(2, 0, 3, 1, 4, 5)
        every = every.reshape(
            every.shape[0], every.shape[1] * every.shape[2], -1, every.shape[5]
        )
        values = lax.dynamic_slice_in_dim(every, lax.axis_index("col") * share, share, 2)
    return values


def pair_of(later, earlier):
    return later * (later - 1) // 2 + earlier


def per_device(
    rhs_sub,
    rhs_top,
    lower_sub,
    lower_link,
    lower_top,
    inv_sub,
    inv_top,
    mask_sub,
    mask_link,
    mask_top,
):
    subs = inv_sub.shape[1]
    tops = inv_top.shape[0]
    col_blocks = lower_top.shape[2]
    share = rhs_top.shape[2]
    levels = subs + tops
    inverse = [inv_sub[0, l] for l in range(subs)] + [inv_top[t] for t in range(tops)]
    rhs = [rhs_sub[0, l] for l in range(subs)] + [rhs_top[t] for t in range(tops)]

    def factor(a, b):
        if a < subs:
            p = pair_of(a, b)
            return scaled(lower_sub[0, p], mask_sub[0, p], inverse[a])
        if b < subs:
            return scaled(lower_link[0, a - subs], mask_link[0, a - subs], inverse[a])
        p = pair_of(a - subs, b - subs)
        return scaled(lower_top[p], mask_top[p], inverse[a])

    scaled_rhs = jnp.stack(
        [
            jnp.einsum("ind,ide->ine", v.astype(BF), w, preferred_element_type=F32).astype(BF)
            for v, w in zip(rhs, inverse)
        ]
    )
    owned = into_owner_layout(scaled_rhs, col_blocks)
    base = [owned[l].astype(F32) for l in range(levels)]
    pairs = [(a, b) for a in range(levels) for b in range(a) if a < subs or b >= subs - 1]
    gathered = {ab: row_gather(factor(*ab)) for ab in pairs}

    solved = []
    for a in range(levels):
        value = base[a]
        near = [b for b in range(a) if (a, b) in gathered]
        own = [b for b in near if a < subs or b >= subs]
        cross = [b for b in near if b not in own]
        for group, across in ((own, False), (cross, True)):
            if group:
                parts = sum(spread(solved[b].astype(BF), gathered[a, b]) for b in group)
                total = to_owners(parts[:, None], 1)[0]
                if across:
                    both = lax.all_gather(total.astype(BF), "gz").astype(F32)
                    total = jnp.sum(both, axis=0)
                value = value - total
        solved.append(value)

    back = [None] * levels
    arrived = {}
    for b in reversed(range(levels)):
        value = solved[b]
        for a in range(b + 1, levels):
            if (a, b) in gathered:
                value = value - collect(arrived[a], 0, gathered[a, b])
        back[b] = value.astype(BF)
        if b:
            arrived[b] = from_owners(back[b][None])

    answers = []
    for l in range(levels):
        rows_back = from_owner_layout(back[l][None], share)[0]
        answers.append(
            jnp.einsum("ind,ibd->inb", rows_back, inverse[l], preferred_element_type=F32)
        )
    return jnp.stack(answers[:subs])[None], jnp.stack(answers[subs:])


def solution(mesh):
    return jax.shard_map(
        per_device,
        mesh=mesh,
        in_specs=(
            P("gz", None, "row", "col", None),
            P(None, "row", "col", None),
            P("gz", None, "row", "col", None, None),
            P("gz", None, "row", "col", None, None),
            P(None, "row", "col", None, None),
            P("gz", None, "row", None, None),
            P(None, "row", None, None),
            P("gz", None, "row", "col"),
            P("gz", None, "row", "col"),
            P(None, "row", "col"),
        ),
        out_specs=(P("gz", None, "row", "col", None), P(None, "row", "col", None)),
        check_vma=False,
    )
```

```python
import jax
import jax.numpy as jnp
from jax import lax
from jax.sharding import PartitionSpec as P

BF = jnp.bfloat16
F32 = jnp.float32


def ring_from(values, axis, step):
    size = lax.axis_size(axis)
    if step == 0:
        return values
    return lax.ppermute(values, axis, [((d + step) % size, d) for d in range(size)])


def rolled(stack, start):
    size = stack.shape[0]
    return lax.dynamic_slice_in_dim(jnp.concatenate([stack, stack]), start % size, size, 0)


def row_gather(block):
    return [ring_from(block, "row", p) for p in range(lax.axis_size("row"))]


def scaled(lower, pattern, inverse):
    kept = lower * pattern.astype(BF)[:, :, None, None]
    return jnp.einsum("ijbd,ide->ijbe", kept, inverse, preferred_element_type=F32).astype(BF)


def spread(vectors, gathered):
    return jnp.stack(
        [jnp.einsum("jnb,ijbd->ind", vectors, g, preferred_element_type=F32) for g in gathered]
    )


def to_owners(parts, levels):
    rows, cols = lax.axis_size("row"), lax.axis_size("col")
    r, j = lax.axis_index("row"), lax.axis_index("col")
    parts = parts.astype(BF)
    if rows == cols:
        total = lax.dynamic_index_in_dim(parts, (j - r) % rows, 0, False).astype(F32)
        for s in range(1, cols):
            send = lax.dynamic_index_in_dim(parts, (j + s - r) % rows, 0, False)
            got = lax.ppermute(send, "col", [(d, (d + s) % cols) for d in range(cols)])
            total = total + got.astype(F32)
        return total
    natural = rolled(parts, rows - r)
    natural = jnp.moveaxis(natural, 1, 2)
    natural = natural.reshape((cols, -1) + natural.shape[2:])
    got = lax.all_to_all(natural, "col", 0, 0, tiled=True)
    return jnp.moveaxis(jnp.sum(got.astype(F32), axis=0), 1, 0)


def from_owners(vectors):
    rows, cols = lax.axis_size("row"), lax.axis_size("col")
    r, j = lax.axis_index("row"), lax.axis_index("col")
    if rows == cols:
        stack = jnp.stack([ring_from(vectors, "col", s) for s in range(cols)])
        return rolled(stack, r - j)
    stack = lax.all_gather(vectors, "col", axis=1, tiled=True)
    stack = stack.reshape((stack.shape[0], rows, -1) + stack.shape[2:])
    return rolled(jnp.moveaxis(stack, 1, 0), r)


def collect(rel, index, gathered):
    total = 0.0
    for p, g in enumerate(gathered):
        total = total + jnp.einsum("knd,kjbd->jnb", rel[p, index], g, preferred_element_type=F32)
    return total


def owner_pairs(rows, cols):
    wide = cols // rows
    return [
        (a * cols + c, (c % rows) * cols + a * wide + c // rows)
        for a in range(rows)
        for c in range(cols)
    ]


def into_owner_layout(values, col_blocks):
    rows, cols = lax.axis_size("row"), lax.axis_size("col")
    if rows != cols:
        c = lax.axis_index("col")
        values = lax.all_gather(values, "col", axis=2, tiled=True)
        n = values.shape[2] // rows
        values = lax.dynamic_slice_in_dim(values, (c // rows) * col_blocks, col_blocks, 1)
        values = lax.dynamic_slice_in_dim(values, (c % rows) * n, n, 2)
    return lax.ppermute(values, ("row", "col"), owner_pairs(rows, cols))


def from_owner_layout(values, share):
    rows, cols = lax.axis_size("row"), lax.axis_size("col")
    values = lax.ppermute(values, ("row", "col"), [(b, a) for a, b in owner_pairs(rows, cols)])
    if rows != cols:
        every = lax.all_gather(values, "col", axis=0)
        every = every.reshape((cols // rows, rows) + every.shape[1:])
        every = every.transpose(2, 0, 3, 1, 4, 5)
        every = every.reshape(
            every.shape[0], every.shape[1] * every.shape[2], -1, every.shape[5]
        )
        values = lax.dynamic_slice_in_dim(every, lax.axis_index("col") * share, share, 2)
    return values


def pair_of(later, earlier):
    return later * (later - 1) // 2 + earlier


def composite(direct, first, second):
    rows = lax.axis_size("row")
    r, j = lax.axis_index("row"), lax.axis_index("col")
    total = 0.0
    for p in range(rows):
        part = lax.dynamic_index_in_dim(second, (r + p - j) % rows, 0, False)
        total = total + jnp.einsum("kjbd,ikde->ijbe", first[p], part, preferred_element_type=F32)
    return (direct.astype(F32) - total).astype(BF)


def col_gather(block):
    return jnp.stack([ring_from(block, "col", s) for s in range(lax.axis_size("col"))])


def packed_row_gather(blocks):
    got = row_gather(jnp.stack(blocks))
    return [[g[m] for g in got] for m in range(len(blocks))]


def solve_by_tiers(base, factor, share):
    x0, r1, r2, r3, r4 = base
    m10, m21, m20 = factor(1, 0), factor(2, 1), factor(2, 0)
    k0, k1, top = factor(3, 2), factor(4, 2), factor(4, 3)
    g10, gk0 = packed_row_gather([m10, k0])
    g21, gtop = packed_row_gather([m21, top])
    g20 = row_gather(composite(m20, g10, col_gather(m21)))
    gk1 = row_gather(composite(k1, gk0, col_gather(top)))
    parts = jnp.stack(
        [spread(x0, g10), spread(r1, g21) + spread(x0, g20)], axis=1
    )
    moved = to_owners(parts, 2)
    x1 = r1.astype(F32) - moved[0]
    x2 = r2.astype(F32) - moved[1]
    h2 = x2.astype(BF)
    portion = 1.0 / lax.axis_size("gz")
    parts = jnp.stack(
        [spread(h2, gk0), spread(h2, gk1) + portion * spread(r3, gtop)], axis=1
    )
    both = lax.all_gather(to_owners(parts, 2).astype(BF), "gz").astype(F32)
    moved = jnp.sum(both, axis=0)
    x3 = r3.astype(F32) - moved[0]
    u4 = (r4.astype(F32) - moved[1]).astype(BF)
    h1 = x1.astype(BF)
    rel = from_owners(jnp.stack([u4, x3.astype(BF), h1]))
    u3 = (x3 - collect(rel, 0, gtop)).astype(BF)
    u2 = (x2 - collect(rel, 1, gk0) - collect(rel, 0, gk1)).astype(BF)
    late = from_owners(u2[None])
    early = from_owner_layout(jnp.stack([u2, u3, u4]), share)
    u1 = (x1 - collect(late, 0, g21)).astype(BF)
    u0 = (x0.astype(F32) - collect(rel, 2, g10) - collect(late, 0, g20)).astype(BF)
    last = from_owner_layout(jnp.stack([u0, u1]), share)
    return [last[0], last[1], early[0], early[1], early[2]]


def solve_by_level(base, factor, subs, share):
    levels = len(base)
    base = [v.astype(F32) for v in base]
    pairs = [(a, b) for a in range(levels) for b in range(a) if a < subs or b >= subs - 1]
    gathered = {ab: row_gather(factor(*ab)) for ab in pairs}

    solved = []
    for a in range(levels):
        value = base[a]
        near = [b for b in range(a) if (a, b) in gathered]
        own = [b for b in near if a < subs or b >= subs]
        cross = [b for b in near if b not in own]
        for group, across in ((own, False), (cross, True)):
            if group:
                parts = sum(spread(solved[b].astype(BF), gathered[a, b]) for b in group)
                total = to_owners(parts[:, None], 1)[0]
                if across:
                    both = lax.all_gather(total.astype(BF), "gz").astype(F32)
                    total = jnp.sum(both, axis=0)
                value = value - total
        solved.append(value)

    back = [None] * levels
    arrived = {}
    for b in reversed(range(levels)):
        value = solved[b]
        for a in range(b + 1, levels):
            if (a, b) in gathered:
                value = value - collect(arrived[a], 0, gathered[a, b])
        back[b] = value.astype(BF)
        if b:
            arrived[b] = from_owners(back[b][None])

    return [from_owner_layout(back[l][None], share)[0] for l in range(levels)]


def per_device(
    rhs_sub,
    rhs_top,
    lower_sub,
    lower_link,
    lower_top,
    inv_sub,
    inv_top,
    mask_sub,
    mask_link,
    mask_top,
):
    subs = inv_sub.shape[1]
    tops = inv_top.shape[0]
    col_blocks = lower_top.shape[2]
    share = rhs_top.shape[2]
    levels = subs + tops
    inverse = [inv_sub[0, l] for l in range(subs)] + [inv_top[t] for t in range(tops)]
    rhs = [rhs_sub[0, l] for l in range(subs)] + [rhs_top[t] for t in range(tops)]

    def factor(a, b):
        if a < subs:
            p = pair_of(a, b)
            return scaled(lower_sub[0, p], mask_sub[0, p], inverse[a])
        if b < subs:
            return scaled(lower_link[0, a - subs], mask_link[0, a - subs], inverse[a])
        p = pair_of(a - subs, b - subs)
        return scaled(lower_top[p], mask_top[p], inverse[a])

    scaled_rhs = jnp.stack(
        [
            jnp.einsum("ind,ide->ine", v.astype(BF), w, preferred_element_type=F32).astype(BF)
            for v, w in zip(rhs, inverse)
        ]
    )
    owned = into_owner_layout(scaled_rhs, col_blocks)
    base = [owned[l] for l in range(levels)]
    if subs == 3 and tops == 2 and lax.axis_size("row") == lax.axis_size("col"):
        native = solve_by_tiers(base, factor, share)
    else:
        native = solve_by_level(base, factor, subs, share)

    answers = []
    for l in range(levels):
        answers.append(
            jnp.einsum("ind,ibd->inb", native[l], inverse[l], preferred_element_type=F32)
        )
    return jnp.stack(answers[:subs])[None], jnp.stack(answers[subs:])


def solution(mesh):
    return jax.shard_map(
        per_device,
        mesh=mesh,
        in_specs=(
            P("gz", None, "row", "col", None),
            P(None, "row", "col", None),
            P("gz", None, "row", "col", None, None),
            P("gz", None, "row", "col", None, None),
            P(None, "row", "col", None, None),
            P("gz", None, "row", None, None),
            P(None, "row", None, None),
            P("gz", None, "row", "col"),
            P("gz", None, "row", "col"),
            P(None, "row", "col"),
        ),
        out_specs=(P("gz", None, "row", "col", None), P(None, "row", "col", None)),
        check_vma=False,
    )
```
